32 devices in a mesh: groups: 2 (over x), blk: 4 (over y, core), col: 4 (over z).
Axes of the slice: x: 2, y: 2, z: 4, core: 2. Of those that a mesh axis runs over, the one named last changes fastest.
Arguments:
- pair_block: bfloat16 [4096, 16384], P(('groups', 'blk'), 'col'), parts along dimension 0, may hold values from -1.5 to 1.5
- occ_energy: float32 [2], P('groups'), parts along dimension 0, may hold values from -1.5 to -0.3
- virt_energy: float32 [4096], P('groups'), parts along dimension 0, may hold values from 0.2 to 3
- frequency: float32 [2], P('groups'), parts along dimension 0, may hold values from 0.2 to 2
Outputs:
- dielectric: float32 [32768, 16384], P(('groups', 'col'), 'blk'), parts along dimension 0
The draws below stay inside these ranges and needn't reach their ends.
There are 2 independent parts, one for each index of `groups`. The reference program is written for one: setup_inputs(seed, part) draws one part's arguments, and reference() takes and returns one part's arrays. A program takes and returns all parts, laid end to end along the dimension named above; each array names one. Nothing has to cross between parts.
All inputs are finite; a program needn't handle non-finite values.
Results may differ from the reference program's by a relative error of at most 0.0027.
Values may be sent and summed in bfloat16 or wider, within the bound.
No kernel may reach another device: no remote copies, remote signals or barrier semaphores. Data moves between devices by JAX's collectives and lax.ppermute only.
A program may use at most 192 MiB of HBM per device.

```python
import math
import jax
import jax.numpy as jnp
from jax import lax

NAUX = 16384
NVIRT = 2048
NOCC = 1
NPAIR = 2048


def block_scale(rng, extent, split, low, largest):
    def one(dim, shards_of):
        steps = jax.random.uniform(jax.random.fold_in(jax.random.fold_in(rng, 6), dim), (shards_of,), jnp.float32, low / len(split), largest / len(split))
        return jnp.repeat(jnp.exp(steps), extent[dim] // shards_of).reshape((-1,) + (1,) * (len(extent) - dim - 1))

    level = one(*split[0])
    for cut in split[1:]:
        level = level * one(*cut)
    return level


def gaussian(own_key, shape, scale, limit, shards=(), held_as=jnp.bfloat16):
    values = scale * jax.random.normal(own_key, shape, jnp.float32)
    if shards:
        values = values * block_scale(own_key, shape, shards, -0.22, 0.18)
    return jnp.clip(values, -limit, limit).astype(held_as)


def setup_inputs(seed: int = 0, part: int = 0) -> dict:
    streams_of = jax.random.split(jax.random.key(seed), 5)
    part_splits = jax.random.split(jax.random.fold_in(streams_of[4], part), 5)
    pair_block = gaussian(part_splits[0], (NPAIR, NAUX), (0.7 * NPAIR ** -0.25), 1.5, ((0, 4), (1, 4)))
    occ_energy = jnp.clip(jax.random.uniform(part_splits[1], (NOCC,), jnp.float32, -1.5, -0.3), -1.5, -0.3)
    virt_energy = jnp.clip(jnp.exp(jax.random.uniform(part_splits[2], (NVIRT,), jnp.float32, math.log(0.2), math.log(3.0))), 0.2, 3.0)
    frequency = jnp.clip(jnp.exp(jax.random.uniform(part_splits[3], (1,), jnp.float32, math.log(0.2), math.log(2.0))), 0.2, 2.0)
    return {"pair_block": pair_block, "occ_energy": occ_energy, "virt_energy": virt_energy, "frequency": frequency}


def reference(pair_block, occ_energy, virt_energy, frequency):
    gap = (virt_energy[None, :] - occ_energy[:, None]).reshape(-1)
    weights = 2.0 * gap / (gap * gap + frequency[0] * frequency[0])
    scaled = (pair_block.astype(jnp.float32) * weights[:, None]).astype(jnp.bfloat16)
    return lax.dot_general(scaled, pair_block, (((0,), (0,)), ((), ())), preferred_element_type=jnp.float32)
```

```python
import jax
import jax.numpy as jnp
from jax import lax
from jax.sharding import PartitionSpec as P

CHUNKS = 8
LAG = 2


def pair_weights(occ_energy, virt_energy, frequency):
    gap = (virt_energy[None, :] - occ_energy[:, None]).reshape(-1)
    return 2.0 * gap / (gap * gap + frequency[0] * frequency[0])


def shards(pair_block, occ_energy, virt_energy, frequency):
    weights = pair_weights(occ_energy, virt_energy, frequency)
    row_full = lax.all_gather(pair_block, "col", axis=1, tiled=True)
    column_slab = lax.all_to_all(row_full, "blk", split_axis=1, concat_axis=0, tiled=True)
    scaled = (
        lax.all_gather(pair_block, "blk", axis=0, tiled=True).astype(jnp.float32) * weights[:, None]
    ).astype(jnp.bfloat16)
    return lax.dot_general(
        scaled, column_slab, (((0,), (0,)), ((), ())), preferred_element_type=jnp.float32
    )


def line_shards(size):
    half = size // 2
    axes = ("blk", "col")

    def device(b, z):
        return b * size + z

    def step_of(b):
        return 1 if b < half else -1

    def other(b):
        return b ^ half

    def send(x, pairs):
        return lax.ppermute(x, axes, pairs)

    core_swap = [(device(b, z), device(b ^ 1, z)) for b in range(size) for z in range(size)]
    y_swap = [(device(b, z), device(other(b), z)) for b in range(size) for z in range(size)]
    side = [
        (device(b, b), device(b, b - step_of(b)))
        for b in range(size)
        if 0 <= b - step_of(b) < size
    ]

    def hops(first, carrier, live):
        step = step_of(first)
        out = []
        z = first
        hop = 0
        while 0 <= z + step < size:
            if live(hop):
                out.append((device(carrier, z), device(carrier, z + step)))
            z += step
            hop += 1
        return out

    def body(pair_block, occ_energy, virt_energy, frequency):
        rows, cols = pair_block.shape
        width = cols // CHUNKS
        b = lax.axis_index("blk")
        z = lax.axis_index("col")
        away = jnp.where(b < half, z - b, b - z)
        order = jnp.stack([b, b ^ 1, b ^ half ^ 1, b ^ half])
        weights = pair_weights(occ_energy, virt_energy, frequency)
        weights = jnp.take(weights.reshape(size, rows), order, axis=0).reshape(-1)

        def cut(x, j):
            return lax.slice_in_dim(x, j * width, (j + 1) * width, axis=1)

        last = CHUNKS + (size - 2) * LAG
        ready = LAG * size
        held = {("own", j): cut(pair_block, j) for j in range(CHUNKS)}
        held["all"] = pair_block
        held["weights"] = weights.reshape(size, rows)
        held["zero"] = 0.0 * frequency[0]
        swaps = {}
        for j in range(CHUNKS):
            swaps.setdefault((j + 1) // 2, []).append(j)

        def local(j):
            return jnp.concatenate([held["own", j], cut(held["mate"], j), held["diag", j]], 0)

        def feed(fresh, name, r, source):
            if r >= CHUNKS:
                return held[name, r - LAG]
            return fresh(r) if r < LAG else jnp.where(z == source, fresh(r), held[name, r - LAG])

        def pairs_at(r, shift):
            return [
                p
                for c in range(size)
                for p in hops(c ^ shift, c, lambda hop: 0 <= r - hop * LAG < CHUNKS)
            ]

        def place(x, i, j=0):
            part = x.astype(jnp.float32) * held["weights"][i][:, None]
            held["lhs"] = lax.dynamic_update_slice(
                held["lhs"], part.astype(jnp.bfloat16), (i * rows, j * width)
            )

        flight = {}
        placed = set()
        for r in range(ready + CHUNKS):
            held.update(flight.pop(r - LAG, {}))
            names = list(held)
            held = dict(zip(names, lax.optimization_barrier([held[n] for n in names])))
            new = {}
            m = r - LAG
            if 0 <= m < last:
                new["main", m] = send(feed(local, "main", m, b), pairs_at(m, 0))
                cross = [(d, device(other(d // size), d % size)) for _, d in pairs_at(m, half)]
                new["cross", m] = send(held["detour", m], cross)
            if r < last:
                new["detour", r] = send(
                    feed(lambda j: held["own", j], "detour", r, b ^ half), pairs_at(r, half)
                )
            if 0 <= m < CHUNKS:
                new["side", m] = send(jnp.concatenate([local(m), held["over", m]], 0), side)
            if r == 0:
                new["mate"] = send(held["all"], core_swap)
            for j in range(CHUNKS):
                if ("over", j) in held and ("diag", j) not in held and j >= LAG * 2:
                    if ("diag", j) not in flight.get(r - 1, {}):
                        new["diag", j] = send(held["over", j], core_swap)
            for j in swaps.get(r, []):
                new["over", j] = send(held["own", j], y_swap)
                if j < LAG * 2:
                    new["diag", j] = send(new["over", j], core_swap)
            flight[r] = new
            if r == 4:
                held["lhs"] = jnp.broadcast_to(held["zero"].astype(jnp.bfloat16), (size * rows, cols))
                place(held["all"], 0)
            if r == 5:
                place(held["mate"], 1)
            if r == 6:
                held["out"] = jnp.broadcast_to(held["zero"], (cols, cols))
            for i, name in ((2, "diag"), (3, "over")) if r > 4 else ():
                for j in range(CHUNKS):
                    if (name, j) in held and (name, j) not in placed:
                        placed.add((name, j))
                        place(held[name, j], i, j)
            j = r - ready
            if j < 0:
                continue
            right = jnp.where(
                away == 0, jnp.concatenate([local(j), held["over", j]], 0), held["side", j]
            )
            for d in range(1, size):
                t = j + (d - 1) * LAG
                far = jnp.concatenate([held["main", t], held["cross", t]], 0)
                right = jnp.where(away == d, far, right)
            piece = lax.dot_general(
                held["lhs"], right, (((0,), (0,)), ((), ())), preferred_element_type=jnp.float32
            )
            held["out"] = lax.dynamic_update_slice(held["out"], piece, (0, j * width))
        return held["out"]

    return body


def solution(mesh):
    blk, col = mesh.shape["blk"], mesh.shape["col"]
    return jax.shard_map(
        line_shards(blk) if blk == col == 4 else shards,
        mesh=mesh,
        in_specs=(P(("groups", "blk"), "col"), P("groups"), P("groups"), P("groups")),
        out_specs=P(("groups", "col"), "blk"),
        check_vma=False,
    )
```
